32 devices in a mesh: dp: 32 (over z, y, x, core).
Axes of the slice: x: 2, y: 2, z: 4, core: 2. Of those that a mesh axis runs over, the one named last changes fastest.
Arguments:
- hidden: bfloat16 [24576, 2560], P('dp'), may hold values from -16 to 16
- rotation: bfloat16 [2560, 2560], P('dp'), may hold values from -1 to 1, as said below
- norm_gain: float32 [2, 2560], replicated, may hold values from 0.1 to 1.9
- value_weight: bfloat16 [2, 2560, 1024], P(None, None, 'dp'), may hold values from -0.125 to 0.125
- output_weight: bfloat16 [2, 1024, 2560], P(None, 'dp'), may hold values from -0.1875 to 0.1875
- lengths: int32 [32], replicated, may hold values from 1 to 768, as said below
Outputs:
- rotated_out: bfloat16 [24576, 2560], P('dp')
- calib_loss: float32 [], replicated
The draws below stay inside these ranges and needn't reach their ends.
Inputs may be any that keep to these rules, and one draw needn't show every extreme that they name: `lengths`: some device has all of its 768 rows live. `rotation`: an orthogonal matrix rounded to bfloat16.
All inputs are finite; a program needn't handle non-finite values.
Results may differ from the reference program's by a relative error of at most 0.0088.
Values may be sent and summed in bfloat16 or wider, within the bound.
A program may use at most 192 MiB of HBM per device.

```python
import jax
import jax.numpy as jnp
from jax import lax

D = 2560
E = 1024
BLOCK = 256
SLOTS = 3
LAYERS = 2
ROWS_DEV = 768
ROWS = 24576
N_DP = 32


def draw_hidden(key, part):
    noise_key, factor_key = jax.random.split(key)
    samples = jax.random.normal(noise_key, (ROWS, D), jnp.float32)
    row_factor = jnp.exp(jax.random.uniform(factor_key, (ROWS, 1), jnp.float32, -0.35, 0.35))
    rising = 0.5 + jnp.arange(ROWS, dtype=jnp.float32)[:, None] / ROWS
    return jnp.clip(samples * rising * row_factor, -16.0, 16.0).astype(jnp.bfloat16)


def draw_rotation(key, part):
    samples = jax.random.normal(key, (D, D), jnp.float32)
    orthogonal, triangle = jnp.linalg.qr(samples)
    return orthogonal.astype(jnp.bfloat16)


def draw_lengths(key, part):
    full_span = SLOTS * BLOCK
    draw_key, pick_key = jax.random.split(key)
    uniform_ints = jax.random.randint(draw_key, (N_DP,), 0, full_span)
    skewed = 1 + uniform_ints * uniform_ints // full_span
    chosen = jax.random.randint(pick_key, (), 0, N_DP)
    return jnp.where(jnp.arange(N_DP) == chosen, full_span, skewed).astype(jnp.int32)


def block_levels(key, dims, cuts, smallest, top_value):
    factor_of = 1.0
    for dim, blocks in cuts:
        draws = jax.random.uniform(jax.random.fold_in(jax.random.fold_in(key, 6), dim), (blocks,), jnp.float32, smallest / len(cuts), top_value / len(cuts))
        factor_of = factor_of * jnp.repeat(jnp.exp(draws), dims[dim] // blocks).reshape((-1,) + (1,) * (len(dims) - 1 - dim))
    return factor_of


def bell_draw(own_key, extent, deviation, bound, cuts=(), kind=jnp.bfloat16):
    loudness = block_levels(own_key, extent, cuts, -0.22, 0.18) if cuts else 1.0
    drawn = jax.random.normal(own_key, extent, jnp.float32) * deviation * loudness
    return jnp.minimum(jnp.maximum(drawn, -bound), bound).astype(kind)


def setup_inputs(seed: int = 0) -> dict:
    key_list = jax.random.split(jax.random.key(seed), 7)
    return {
        "hidden": draw_hidden(jax.random.fold_in(key_list[6], 71), 0),
        "rotation": draw_rotation(jax.random.fold_in(key_list[6], 71), 0),
        "norm_gain": jnp.clip(1.0 + 0.18 * jax.random.normal(key_list[2], (LAYERS, D), jnp.float32), 0.1, 1.9),
        "value_weight": bell_draw(key_list[3], (LAYERS, D, E), D ** -0.5, 0.125, ((2, 32),)),
        "output_weight": bell_draw(key_list[4], (LAYERS, E, D), E ** -0.5, 0.1875, ((1, 32),)),
        "lengths": draw_lengths(jax.random.fold_in(key_list[6], 71), 0),
    }


EPS_NORM = 1e-06
EPS_SCALE = 1e-06
CLIP_RATIO = 0.9
TWO_PI = 6.283185307179586

def soft_round(values):
    return values - jnp.sin(TWO_PI * values) / TWO_PI

def fake_quant(values, step_size):
    return soft_round(jnp.clip(values / step_size, -8.0, 7.0)) * step_size

def quant_columns(matrix):
    step_size = lax.optimization_barrier(jnp.max(jnp.abs(matrix), axis=0)) / 7.0 + EPS_SCALE
    return fake_quant(matrix, step_size[None, :]).astype(jnp.bfloat16)

def reference(hidden, rotation, norm_gain, value_weight, output_weight, lengths):
    positions = lax.broadcasted_iota(jnp.int32, (N_DP, ROWS_DEV), 1)
    live_rows = positions < lengths[:, None]
    count = jnp.sum(lengths).astype(jnp.float32)
    blocks = hidden.reshape(N_DP, ROWS_DEV, D)
    resid = lax.map(lambda block_rows: jnp.dot(block_rows.astype(jnp.float32), rotation.astype(jnp.float32), preferred_element_type=jnp.float32), blocks)
    loss_sum = jnp.zeros((), jnp.float32)
    for layer_number in range(LAYERS):
        scaled = (norm_gain[layer_number][:, None] * value_weight[layer_number].astype(jnp.float32)).astype(jnp.bfloat16)
        rotated_v = lax.dot_general(rotation.astype(jnp.float32), scaled.astype(jnp.float32), (((0,), (0,)), ((), ())), preferred_element_type=jnp.float32)
        value_q = quant_columns(rotated_v)
        rotated_o = jnp.dot(output_weight[layer_number].astype(jnp.float32), rotation.astype(jnp.float32), preferred_element_type=jnp.float32)
        output_q = quant_columns(rotated_o)

        def first_pass(operands):
            residual, live_mask = operands
            mean_sq = lax.optimization_barrier(jnp.mean(residual * residual, axis=1))
            normed = residual * lax.rsqrt(mean_sq + EPS_NORM)[:, None]
            step_size = CLIP_RATIO * lax.optimization_barrier(jnp.max(jnp.abs(normed), axis=1)) / 7.0 + EPS_SCALE
            act_f = fake_quant(normed, step_size[:, None])
            act_err = lax.optimization_barrier(jnp.sum((act_f - normed) * (act_f - normed), axis=1))
            mixed = jnp.dot(act_f.astype(jnp.bfloat16).astype(jnp.float32), value_q.astype(jnp.float32), preferred_element_type=jnp.float32)
            channel_top = lax.optimization_barrier(jnp.max(jnp.where(live_mask[:, None], jnp.abs(mixed), 0.0), axis=0))
            return (mean_sq, act_err, mixed, channel_top)
        mean_sq, act_err, mixed, channel_top = lax.map(first_pass, (resid, live_rows))
        vrange = lax.optimization_barrier(jnp.max(channel_top, axis=0))
        mix_step = CLIP_RATIO * vrange / 7.0 + EPS_SCALE

        def second_pass(operands):
            residual, mixed_rows = operands
            mix_f = fake_quant(mixed_rows, mix_step[None, :])
            mix_err = lax.optimization_barrier(jnp.sum((mix_f - mixed_rows) * (mix_f - mixed_rows), axis=1))
            updated = residual + jnp.dot(mix_f.astype(jnp.bfloat16).astype(jnp.float32), output_q.astype(jnp.float32), preferred_element_type=jnp.float32)
            return (updated, mix_err)
        resid, mix_err = lax.map(second_pass, (resid, mixed))
        loss_sum = loss_sum + jnp.sum(jnp.where(live_rows, mean_sq * (act_err + mix_err), 0.0))
    rotated_out = jnp.where(live_rows[:, :, None], resid, 0.0).astype(jnp.bfloat16).reshape(ROWS, D)
    return (rotated_out, loss_sum / count)
```

```python
import functools

import jax
import jax.numpy as jnp
from jax import lax
from jax.experimental import pallas as pl
from jax.experimental.pallas import tpu as pltpu
from jax.sharding import PartitionSpec as P

BLOCK = 256
CHUNK = 16
TILE = 512
VMEM_LIMIT = 60 * 1024 * 1024

EPS_NORM = 1e-06
EPS_SCALE = 1e-06
CLIP_RATIO = 0.9
POLY = (0.9999997571452157, -2.579687436847881, 2.6673586060553345, -1.5145036626283546, 0.48039577352173)


def soft_round(values):
    r = values - jnp.round(values)
    u = r * r
    p = jnp.float32(POLY[-1])
    for c in POLY[-2::-1]:
        p = p * u + jnp.float32(c)
    return values - p * (r - 4.0 * (r * u))


def fake_quant(values, step_size):
    inv = 1.0 / step_size
    return soft_round(jnp.clip(values * inv, -8.0, 7.0)) * step_size


def weight_kernel(v_rows, o_rows, layers, w_ref, r_ref, vq_ref, o_ref, top_ref, acc):
    j = pl.program_id(0)
    n = r_ref.shape[1]
    at = pl.ds(pl.multiple_of(j * n, n), n)
    prod = jnp.dot(w_ref[...], r_ref[...], preferred_element_type=jnp.float32)
    acc[:, at] = prod[:v_rows]
    o_ref[...] = prod[v_rows:]
    per = o_rows // layers
    for l in range(layers):
        lo = v_rows + l * per
        top_ref[l : l + 1, :] = jnp.max(jnp.abs(prod[lo : lo + per]), axis=0, keepdims=True)

    @pl.when(j == pl.num_programs(0) - 1)
    def _():
        def body(i, _):
            rows = pl.ds(pl.multiple_of(i * CHUNK, CHUNK), CHUNK)
            x = acc[rows, :]
            step = jnp.max(jnp.abs(x), axis=1, keepdims=True) / 7.0 + EPS_SCALE
            vq_ref[rows, :] = fake_quant(x, step).astype(jnp.bfloat16)
            return 0

        lax.fori_loop(0, v_rows // CHUNK, body, 0)


def rotate_weights(joined, rotation, v_rows, o_rows, layers):
    width = rotation.shape[1]
    depth = rotation.shape[0]
    return pl.pallas_call(
        functools.partial(weight_kernel, v_rows, o_rows, layers),
        name="rotate_weights",
        grid=(width // TILE,),
        in_specs=[
            pl.BlockSpec(joined.shape, lambda j: (0, 0)),
            pl.BlockSpec((depth, TILE), lambda j: (0, j)),
        ],
        out_specs=[
            pl.BlockSpec((v_rows, width), lambda j: (0, 0)),
            pl.BlockSpec((o_rows, TILE), lambda j: (0, j)),
            pl.BlockSpec((layers, TILE), lambda j: (0, j)),
        ],
        out_shape=[
            jax.ShapeDtypeStruct((v_rows, width), jnp.bfloat16),
            jax.ShapeDtypeStruct((o_rows, width), jnp.float32),
            jax.ShapeDtypeStruct((layers, width), jnp.float32),
        ],
        scratch_shapes=[pltpu.VMEM((v_rows, width), jnp.float32)],
        compiler_params=pltpu.CompilerParams(vmem_limit_bytes=VMEM_LIMIT),
        cost_estimate=pl.CostEstimate(
            flops=2 * joined.shape[0] * depth * width,
            bytes_accessed=2 * depth * width,
            transcendentals=0,
        ),
    )(joined, rotation)


def norm_rows(resid_ref, act_ref, msq_ref, aerr_ref):
    width = resid_ref.shape[1]

    def body(i, _):
        rows = pl.ds(pl.multiple_of(i * CHUNK, CHUNK), CHUNK)
        x = resid_ref[rows, :]
        mean_sq = jnp.sum(x * x, axis=1, keepdims=True) * (1.0 / width)
        inv = lax.rsqrt(mean_sq + EPS_NORM)
        step = CLIP_RATIO * (jnp.max(jnp.abs(x), axis=1, keepdims=True) * inv) / 7.0 + EPS_SCALE
        normed = x * inv
        act = fake_quant(normed, step)
        diff = act - normed
        act_ref[rows, :] = act.astype(jnp.bfloat16)
        msq_ref[rows, :] = mean_sq
        aerr_ref[rows, :] = jnp.sum(diff * diff, axis=1, keepdims=True)
        return 0

    lax.fori_loop(0, resid_ref.shape[0] // CHUNK, body, 0)


def first_kernel(h_ref, r_ref, resid_ref, act_ref, msq_ref, aerr_ref):
    def body(j, _):
        at = pl.ds(pl.multiple_of(j * TILE, TILE), TILE)
        resid_ref[:, at] = jnp.dot(h_ref[...], r_ref[:, at], preferred_element_type=jnp.float32)
        return 0

    lax.fori_loop(0, r_ref.shape[1] // TILE, body, 0)
    norm_rows(resid_ref, act_ref, msq_ref, aerr_ref)


def rows_spec(width):
    return pl.BlockSpec((BLOCK, width), lambda i, *_: (i, 0))


def whole_spec(shape):
    return pl.BlockSpec(shape, lambda i, *_: (0, 0), pipeline_mode=pl.Buffered(1))


def act_shapes(rows, width):
    return [
        jax.ShapeDtypeStruct((rows, width), jnp.float32),
        jax.ShapeDtypeStruct((rows, width), jnp.bfloat16),
        jax.ShapeDtypeStruct((rows, 1), jnp.float32),
        jax.ShapeDtypeStruct((rows, 1), jnp.float32),
    ]


def first_pass(hidden, rotation):
    rows, depth = hidden.shape
    width = rotation.shape[1]
    return pl.pallas_call(
        first_kernel,
        name="rotate_hidden",
        grid=(rows // BLOCK,),
        in_specs=[rows_spec(depth), whole_spec(rotation.shape)],
        out_specs=[rows_spec(width), rows_spec(width), rows_spec(1), rows_spec(1)],
        out_shape=act_shapes(rows, width),
        compiler_params=pltpu.CompilerParams(vmem_limit_bytes=VMEM_LIMIT),
        cost_estimate=pl.CostEstimate(
            flops=2 * rows * depth * width,
            bytes_accessed=2 * depth * width + 8 * rows * width,
            transcendentals=0,
        ),
    )(hidden, rotation)


def mix_kernel(len_ref, act_ref, v_ref, mixed_ref, top_ref):
    i = pl.program_id(0)
    tile = 256
    live = len_ref[0] - i * BLOCK
    mask = lax.broadcasted_iota(jnp.int32, (BLOCK, 1), 0) < live

    @pl.when(i == 0)
    def _():
        top_ref[...] = jnp.zeros_like(top_ref)

    def body(j, _):
        at = pl.ds(pl.multiple_of(j * tile, tile), tile)
        prod = lax.dot_general(
            act_ref[...],
            v_ref[at, :],
            (((1,), (1,)), ((), ())),
            preferred_element_type=jnp.float32,
        )
        mixed_ref[:, at] = prod
        peak = jnp.max(jnp.where(mask, jnp.abs(prod), 0.0), axis=0, keepdims=True)
        top_ref[:, at] = jnp.maximum(top_ref[:, at], peak)
        return 0

    lax.fori_loop(0, v_ref.shape[0] // tile, body, 0)


def mix_pass(own_len, act, values):
    rows, width = act.shape
    channels = values.shape[0]
    return pl.pallas_call(
        mix_kernel,
        name="mix",
        grid_spec=pltpu.PrefetchScalarGridSpec(
            num_scalar_prefetch=1,
            grid=(rows // BLOCK,),
            in_specs=[rows_spec(width), whole_spec(values.shape)],
            out_specs=[
                rows_spec(channels),
                pl.BlockSpec((1, channels), lambda i, *_: (0, 0)),
            ],
        ),
        out_shape=[
            jax.ShapeDtypeStruct((rows, channels), jnp.float32),
            jax.ShapeDtypeStruct((1, channels), jnp.float32),
        ],
        compiler_params=pltpu.CompilerParams(vmem_limit_bytes=VMEM_LIMIT),
        cost_estimate=pl.CostEstimate(
            flops=2 * rows * channels * width,
            bytes_accessed=2 * channels * width + 4 * rows * width,
            transcendentals=0,
        ),
    )(own_len, act, values)


def update_kernel(last, len_ref, mixed_ref, vrange_ref, o_ref, resid_ref, msq_ref, aerr_ref, *rest):
    if last:
        loss_ref, out_ref, mix_buf = rest
    else:
        loss_ref, new_ref, act_ref, nmsq_ref, naerr_ref, mix_buf = rest
    live = len_ref[0] - pl.program_id(0) * BLOCK
    mask = lax.broadcasted_iota(jnp.int32, (BLOCK, 1), 0) < live
    step = CLIP_RATIO * vrange_ref[...] / 7.0 + EPS_SCALE

    def quant(i, _):
        rows = pl.ds(pl.multiple_of(i * CHUNK, CHUNK), CHUNK)
        x = mixed_ref[rows, :]
        mix = fake_quant(x, step)
        diff = mix - x
        mix_buf[rows, :] = mix.astype(jnp.bfloat16)
        loss_ref[rows, :] = jnp.sum(diff * diff, axis=1, keepdims=True)
        return 0

    lax.fori_loop(0, BLOCK // CHUNK, quant, 0)
    loss_ref[...] = jnp.where(mask, msq_ref[...] * (aerr_ref[...] + loss_ref[...]), 0.0)

    def body(j, _):
        at = pl.ds(pl.multiple_of(j * TILE, TILE), TILE)
        new = resid_ref[:, at] + jnp.dot(
            mix_buf[...], o_ref[:, at], preferred_element_type=jnp.float32
        )
        if last:
            out_ref[:, at] = jnp.where(mask, new, 0.0).astype(jnp.bfloat16)
        else:
            new_ref[:, at] = new
        return 0

    lax.fori_loop(0, o_ref.shape[1] // TILE, body, 0)
    if not last:
        norm_rows(new_ref, act_ref, nmsq_ref, naerr_ref)


def update_pass(own_len, mixed, vrange, outputs, resid, msq, aerr, last):
    rows, width = resid.shape
    channels = mixed.shape[1]
    out_specs = [rows_spec(1)]
    out_shape = [jax.ShapeDtypeStruct((rows, 1), jnp.float32)]
    if last:
        out_specs.append(rows_spec(width))
        out_shape.append(jax.ShapeDtypeStruct((rows, width), jnp.bfloat16))
    else:
        out_specs += [rows_spec(width), rows_spec(width), rows_spec(1), rows_spec(1)]
        out_shape += act_shapes(rows, width)
    return pl.pallas_call(
        functools.partial(update_kernel, last),
        name="update",
        grid_spec=pltpu.PrefetchScalarGridSpec(
            num_scalar_prefetch=1,
            grid=(rows // BLOCK,),
            in_specs=[
                rows_spec(channels),
                whole_spec((1, channels)),
                whole_spec(outputs.shape),
                rows_spec(width),
                rows_spec(1),
                rows_spec(1),
            ],
            out_specs=out_specs,
            scratch_shapes=[pltpu.VMEM((BLOCK, channels), jnp.bfloat16)],
        ),
        out_shape=out_shape,
        compiler_params=pltpu.CompilerParams(vmem_limit_bytes=VMEM_LIMIT),
        cost_estimate=pl.CostEstimate(
            flops=2 * rows * channels * width,
            bytes_accessed=2 * channels * width + 12 * rows * width,
            transcendentals=0,
        ),
    )(own_len, mixed, vrange, outputs, resid, msq, aerr)


def per_device(hidden, rotation, norm_gain, value_weight, output_weight, lengths):
    layers = norm_gain.shape[0]
    cols = value_weight.shape[2]
    own_len = lax.dynamic_slice_in_dim(lengths, lax.axis_index("dp"), 1)
    scaled = (norm_gain[:, :, None] * value_weight.astype(jnp.float32)).astype(jnp.bfloat16)
    width = rotation.shape[1]
    depth = value_weight.shape[1]
    joined = jnp.concatenate(
        [
            jnp.swapaxes(scaled, 1, 2).reshape(layers * cols, depth),
            output_weight.reshape(layers * cols, depth),
        ],
        axis=0,
    )
    rotation_full = lax.all_gather(rotation, "dp", axis=0, tiled=True)
    value_q, rotated_o, tops = rotate_weights(
        joined, rotation_full, layers * cols, layers * cols, layers
    )
    tops = lax.pmax(tops, "dp")
    output_q = [
        fake_quant(
            rotated_o[l * cols : (l + 1) * cols], tops[l : l + 1] / 7.0 + EPS_SCALE
        ).astype(jnp.bfloat16)
        for l in range(layers)
    ]
    value_all = []
    output_all = []
    for l in range(layers):
        local_v = value_q[l * cols : (l + 1) * cols]
        if l > 0:
            local_v, _ = lax.optimization_barrier((local_v, output_q[l - 1]))
        value_all.append(lax.all_gather(local_v, "dp", axis=0, tiled=True))
        output_all.append(lax.all_gather(output_q[l], "dp", axis=0, tiled=True))
    hidden, _ = lax.optimization_barrier((hidden, output_q[0]))
    resid, act, msq, aerr = first_pass(hidden, rotation_full)
    loss = jnp.zeros((), jnp.float32)
    for l in range(layers):
        mixed, top = mix_pass(own_len, act, value_all[l])
        vrange = lax.pmax(top, "dp")
        last = l == layers - 1
        res = update_pass(own_len, mixed, vrange, output_all[l], resid, msq, aerr, last)
        loss = loss + jnp.sum(res[0])
        if last:
            out = res[1]
        else:
            resid, act, msq, aerr = res[1:]
    count = jnp.sum(lengths).astype(jnp.float32)
    return (out, lax.psum(loss, "dp") / count)


def solution(mesh):
    return jax.shard_map(
        per_device,
        mesh=mesh,
        in_specs=(P("dp", None), P("dp", None), P(), P(None, None, "dp"), P(None, "dp", None), P()),
        out_specs=(P("dp", None), P()),
        check_vma=False,
    )
```

```python
import functools

import jax
import jax.numpy as jnp
from jax import lax
from jax.experimental import pallas as pl
from jax.experimental.pallas import tpu as pltpu
from jax.sharding import PartitionSpec as P

BLOCK = 256
CHUNK = 16
TILE = 512
VMEM_LIMIT = 60 * 1024 * 1024

EPS_NORM = 1e-06
EPS_SCALE = 1e-06
CLIP_RATIO = 0.9
POLY = (0.9999997571452157, -2.579687436847881, 2.6673586060553345, -1.5145036626283546, 0.48039577352173)


def soft_round(values):
    r = values - jnp.round(values)
    u = r * r
    p = jnp.float32(POLY[-1])
    for c in POLY[-2::-1]:
        p = p * u + jnp.float32(c)
    return values - p * (r - 4.0 * (r * u))


def fake_quant(values, step_size):
    inv = 1.0 / step_size
    return soft_round(jnp.clip(values * inv, -8.0, 7.0)) * step_size


def exchange_kernel(n, total, x_ref, out_ref, slots, send_sem, recv_sem):
    me = lax.axis_index("dp")
    barrier = pltpu.get_barrier_semaphore()

    def greet(k, _):
        pl.semaphore_signal(
            barrier,
            inc=1,
            device_id=(lax.rem(me + k, n),),
            device_id_type=pl.DeviceIdType.MESH,
        )
        return 0

    lax.fori_loop(1, n, greet, 0)
    pl.semaphore_wait(barrier, n - 1)

    def copy_to(peer, slot):
        return pltpu.make_async_remote_copy(
            src_ref=x_ref,
            dst_ref=slots.at[slot],
            send_sem=send_sem.at[peer],
            recv_sem=recv_sem.at[slot],
            device_id=(peer,),
            device_id_type=pl.DeviceIdType.MESH,
        )

    def push(k, _):
        copy_to(lax.rem(me + k, n), me).start()
        return 0

    lax.fori_loop(1, n, push, 0)
    slots[me] = x_ref[...]

    def settle(k, _):
        peer = lax.rem(me + k, n)
        copy = copy_to(peer, peer)
        copy.wait_send()
        copy.wait_recv()
        return 0

    lax.fori_loop(1, n, settle, 0)

    def fold(k, acc):
        return acc + slots[k] if total else jnp.maximum(acc, slots[k])

    out_ref[...] = lax.fori_loop(1, n, fold, slots[0])


def exchange(x, n, collective_id, total=False):
    return pl.pallas_call(
        functools.partial(exchange_kernel, n, total),
        name="exchange",
        in_specs=[pl.BlockSpec(memory_space=pltpu.VMEM)],
        out_specs=pl.BlockSpec(memory_space=pltpu.VMEM),
        out_shape=jax.ShapeDtypeStruct(x.shape, x.dtype),
        scratch_shapes=[
            pltpu.VMEM((n,) + x.shape, x.dtype),
            pltpu.SemaphoreType.DMA((n,)),
            pltpu.SemaphoreType.DMA((n,)),
        ],
        compiler_params=pltpu.CompilerParams(
            collective_id=collective_id, has_side_effects=True, vmem_limit_bytes=VMEM_LIMIT
        ),
        cost_estimate=pl.CostEstimate(flops=0, bytes_accessed=30_000_000, transcendentals=0),
    )(x)


def weight_kernel(v_rows, o_rows, layers, w_ref, r_ref, vq_ref, o_ref, top_ref, acc):
    j = pl.program_id(0)
    n = r_ref.shape[1]
    at = pl.ds(pl.multiple_of(j * n, n), n)
    prod = jnp.dot(w_ref[...], r_ref[...], preferred_element_type=jnp.float32)
    acc[:, at] = prod[:v_rows]
    o_ref[...] = prod[v_rows:]
    per = o_rows // layers
    for l in range(layers):
        lo = v_rows + l * per
        top_ref[l : l + 1, :] = jnp.max(jnp.abs(prod[lo : lo + per]), axis=0, keepdims=True)

    @pl.when(j == pl.num_programs(0) - 1)
    def _():
        def body(i, _):
            rows = pl.ds(pl.multiple_of(i * CHUNK, CHUNK), CHUNK)
            x = acc[rows, :]
            step = jnp.max(jnp.abs(x), axis=1, keepdims=True) / 7.0 + EPS_SCALE
            vq_ref[rows, :] = fake_quant(x, step).astype(jnp.bfloat16)
            return 0

        lax.fori_loop(0, v_rows // CHUNK, body, 0)


def rotate_weights(joined, rotation, v_rows, o_rows, layers):
    width = rotation.shape[1]
    depth = rotation.shape[0]
    return pl.pallas_call(
        functools.partial(weight_kernel, v_rows, o_rows, layers),
        name="rotate_weights",
        grid=(width // TILE,),
        in_specs=[
            pl.BlockSpec(joined.shape, lambda j: (0, 0)),
            pl.BlockSpec((depth, TILE), lambda j: (0, j)),
        ],
        out_specs=[
            pl.BlockSpec((v_rows, width), lambda j: (0, 0)),
            pl.BlockSpec((o_rows, TILE), lambda j: (0, j)),
            pl.BlockSpec((layers, TILE), lambda j: (0, j)),
        ],
        out_shape=[
            jax.ShapeDtypeStruct((v_rows, width), jnp.bfloat16),
            jax.ShapeDtypeStruct((o_rows, width), jnp.float32),
            jax.ShapeDtypeStruct((layers, width), jnp.float32),
        ],
        scratch_shapes=[pltpu.VMEM((v_rows, width), jnp.float32)],
        compiler_params=pltpu.CompilerParams(vmem_limit_bytes=VMEM_LIMIT),
        cost_estimate=pl.CostEstimate(
            flops=2 * joined.shape[0] * depth * width,
            bytes_accessed=2 * depth * width,
            transcendentals=0,
        ),
    )(joined, rotation)


def norm_rows(resid_ref, act_ref, msq_ref, aerr_ref):
    width = resid_ref.shape[1]

    def body(i, _):
        rows = pl.ds(pl.multiple_of(i * CHUNK, CHUNK), CHUNK)
        x = resid_ref[rows, :]
        mean_sq = jnp.sum(x * x, axis=1, keepdims=True) * (1.0 / width)
        inv = lax.rsqrt(mean_sq + EPS_NORM)
        step = CLIP_RATIO * (jnp.max(jnp.abs(x), axis=1, keepdims=True) * inv) / 7.0 + EPS_SCALE
        normed = x * inv
        act = fake_quant(normed, step)
        diff = act - normed
        act_ref[rows, :] = act.astype(jnp.bfloat16)
        msq_ref[rows, :] = mean_sq
        aerr_ref[rows, :] = jnp.sum(diff * diff, axis=1, keepdims=True)
        return 0

    lax.fori_loop(0, resid_ref.shape[0] // CHUNK, body, 0)


def first_kernel(h_ref, r_ref, resid_ref, act_ref, msq_ref, aerr_ref):
    def body(j, _):
        at = pl.ds(pl.multiple_of(j * TILE, TILE), TILE)
        resid_ref[:, at] = jnp.dot(h_ref[...], r_ref[:, at], preferred_element_type=jnp.float32)
        return 0

    lax.fori_loop(0, r_ref.shape[1] // TILE, body, 0)
    norm_rows(resid_ref, act_ref, msq_ref, aerr_ref)


def rows_spec(width):
    return pl.BlockSpec((BLOCK, width), lambda i, *_: (i, 0))


def whole_spec(shape):
    return pl.BlockSpec(shape, lambda i, *_: (0, 0), pipeline_mode=pl.Buffered(1))


def act_shapes(rows, width):
    return [
        jax.ShapeDtypeStruct((rows, width), jnp.float32),
        jax.ShapeDtypeStruct((rows, width), jnp.bfloat16),
        jax.ShapeDtypeStruct((rows, 1), jnp.float32),
        jax.ShapeDtypeStruct((rows, 1), jnp.float32),
    ]


def first_pass(hidden, rotation):
    rows, depth = hidden.shape
    width = rotation.shape[1]
    return pl.pallas_call(
        first_kernel,
        name="rotate_hidden",
        grid=(rows // BLOCK,),
        in_specs=[rows_spec(depth), whole_spec(rotation.shape)],
        out_specs=[rows_spec(width), rows_spec(width), rows_spec(1), rows_spec(1)],
        out_shape=act_shapes(rows, width),
        compiler_params=pltpu.CompilerParams(vmem_limit_bytes=VMEM_LIMIT),
        cost_estimate=pl.CostEstimate(
            flops=2 * rows * depth * width,
            bytes_accessed=2 * depth * width + 8 * rows * width,
            transcendentals=0,
        ),
    )(hidden, rotation)


def mix_kernel(len_ref, act_ref, v_ref, mixed_ref, top_ref):
    i = pl.program_id(0)
    tile = 256
    live = len_ref[0] - i * BLOCK
    mask = lax.broadcasted_iota(jnp.int32, (BLOCK, 1), 0) < live

    @pl.when(i == 0)
    def _():
        top_ref[...] = jnp.zeros_like(top_ref)

    cols = v_ref.shape[1]
    group = tile // cols

    def body(j, _):
        at = pl.ds(pl.multiple_of(j * tile, tile), tile)
        part = v_ref[pl.ds(j * group, group)]
        prod = lax.dot_general(
            act_ref[...],
            part.reshape(tile, part.shape[2]),
            (((1,), (1,)), ((), ())),
            preferred_element_type=jnp.float32,
        )
        mixed_ref[:, at] = prod
        peak = jnp.max(jnp.where(mask, jnp.abs(prod), 0.0), axis=0, keepdims=True)
        top_ref[:, at] = jnp.maximum(top_ref[:, at], peak)
        return 0

    lax.fori_loop(0, v_ref.shape[0] // group, body, 0)


def mix_pass(own_len, act, gathered, layer, cols):
    rows, width = act.shape
    n = gathered.shape[0]
    channels = n * cols
    if cols % 16 == 0:
        values = gathered
        spec = pl.BlockSpec(
            (n, cols, width), lambda i, *_: (0, layer, 0), pipeline_mode=pl.Buffered(1)
        )
    else:
        values = gathered[:, layer * cols : (layer + 1) * cols].reshape(-1, 128, width)
        spec = pl.BlockSpec(values.shape, lambda i, *_: (0, 0, 0), pipeline_mode=pl.Buffered(1))
    return pl.pallas_call(
        mix_kernel,
        name="mix",
        grid_spec=pltpu.PrefetchScalarGridSpec(
            num_scalar_prefetch=1,
            grid=(rows // BLOCK,),
            in_specs=[rows_spec(width), spec],
            out_specs=[
                rows_spec(channels),
                pl.BlockSpec((1, channels), lambda i, *_: (0, 0)),
            ],
        ),
        out_shape=[
            jax.ShapeDtypeStruct((rows, channels), jnp.float32),
            jax.ShapeDtypeStruct((1, channels), jnp.float32),
        ],
        compiler_params=pltpu.CompilerParams(vmem_limit_bytes=VMEM_LIMIT),
        cost_estimate=pl.CostEstimate(
            flops=2 * rows * channels * width,
            bytes_accessed=2 * channels * width + 4 * rows * width,
            transcendentals=0,
        ),
    )(own_len, act, values)


def update_kernel(last, len_ref, mixed_ref, vrange_ref, o_ref, resid_ref, msq_ref, aerr_ref, *rest):
    if last:
        loss_ref, out_ref, mix_buf = rest
    else:
        loss_ref, new_ref, act_ref, nmsq_ref, naerr_ref, mix_buf = rest
    live = len_ref[0] - pl.program_id(0) * BLOCK
    mask = lax.broadcasted_iota(jnp.int32, (BLOCK, 1), 0) < live
    step = CLIP_RATIO * vrange_ref[...] / 7.0 + EPS_SCALE

    def quant(i, _):
        rows = pl.ds(pl.multiple_of(i * CHUNK, CHUNK), CHUNK)
        x = mixed_ref[rows, :]
        mix = fake_quant(x, step)
        diff = mix - x
        mix_buf[rows, :] = mix.astype(jnp.bfloat16)
        loss_ref[rows, :] = jnp.sum(diff * diff, axis=1, keepdims=True)
        return 0

    lax.fori_loop(0, BLOCK // CHUNK, quant, 0)
    loss_ref[...] = jnp.where(mask, msq_ref[...] * (aerr_ref[...] + loss_ref[...]), 0.0)

    def body(j, _):
        at = pl.ds(pl.multiple_of(j * TILE, TILE), TILE)
        new = resid_ref[:, at] + jnp.dot(
            mix_buf[...], o_ref[:, at], preferred_element_type=jnp.float32
        )
        if last:
            out_ref[:, at] = jnp.where(mask, new, 0.0).astype(jnp.bfloat16)
        else:
            new_ref[:, at] = new
        return 0

    lax.fori_loop(0, o_ref.shape[1] // TILE, body, 0)
    if not last:
        norm_rows(new_ref, act_ref, nmsq_ref, naerr_ref)


def update_pass(own_len, mixed, vrange, outputs, resid, msq, aerr, last):
    rows, width = resid.shape
    channels = mixed.shape[1]
    out_specs = [rows_spec(1)]
    out_shape = [jax.ShapeDtypeStruct((rows, 1), jnp.float32)]
    if last:
        out_specs.append(rows_spec(width))
        out_shape.append(jax.ShapeDtypeStruct((rows, width), jnp.bfloat16))
    else:
        out_specs += [rows_spec(width), rows_spec(width), rows_spec(1), rows_spec(1)]
        out_shape += act_shapes(rows, width)
    return pl.pallas_call(
        functools.partial(update_kernel, last),
        name="update",
        grid_spec=pltpu.PrefetchScalarGridSpec(
            num_scalar_prefetch=1,
            grid=(rows // BLOCK,),
            in_specs=[
                rows_spec(channels),
                whole_spec((1, channels)),
                whole_spec(outputs.shape),
                rows_spec(width),
                rows_spec(1),
                rows_spec(1),
            ],
            out_specs=out_specs,
            scratch_shapes=[pltpu.VMEM((BLOCK, channels), jnp.bfloat16)],
        ),
        out_shape=out_shape,
        compiler_params=pltpu.CompilerParams(vmem_limit_bytes=VMEM_LIMIT),
        cost_estimate=pl.CostEstimate(
            flops=2 * rows * channels * width,
            bytes_accessed=2 * channels * width + 12 * rows * width,
            transcendentals=0,
        ),
    )(own_len, mixed, vrange, outputs, resid, msq, aerr)


def per_device(hidden, rotation, norm_gain, value_weight, output_weight, lengths):
    layers = norm_gain.shape[0]
    cols = value_weight.shape[2]
    own_len = lax.dynamic_slice_in_dim(lengths, lax.axis_index("dp"), 1)
    scaled = (norm_gain[:, :, None] * value_weight.astype(jnp.float32)).astype(jnp.bfloat16)
    width = rotation.shape[1]
    depth = value_weight.shape[1]
    joined = jnp.concatenate(
        [
            jnp.swapaxes(scaled, 1, 2).reshape(layers * cols, depth),
            output_weight.reshape(layers * cols, depth),
        ],
        axis=0,
    )
    rotation_full = lax.all_gather(rotation, "dp", axis=0, tiled=True)
    value_q, rotated_o, tops = rotate_weights(
        joined, rotation_full, layers * cols, layers * cols, layers
    )
    n = lax.axis_size("dp")
    tops = exchange(tops, n, 0)
    output_q = [
        fake_quant(
            rotated_o[l * cols : (l + 1) * cols], tops[l : l + 1] / 7.0 + EPS_SCALE
        ).astype(jnp.bfloat16)
        for l in range(layers)
    ]
    value_all = lax.all_gather(value_q, "dp", axis=0, tiled=False)
    output_all = []
    for l in range(layers):
        before = output_all[l - 1] if l > 0 else value_all
        local_o, _ = lax.optimization_barrier((output_q[l], before))
        output_all.append(lax.all_gather(local_o, "dp", axis=0, tiled=True))
    resid, act, msq, aerr = first_pass(hidden, rotation_full)
    loss = jnp.zeros((), jnp.float32)
    for l in range(layers):
        mixed, top = mix_pass(own_len, act, value_all, l, cols)
        vrange = exchange(top, n, 1)
        last = l == layers - 1
        res = update_pass(own_len, mixed, vrange, output_all[l], resid, msq, aerr, last)
        loss = loss + jnp.sum(res[0])
        if last:
            out = res[1]
        else:
            resid, act, msq, aerr = res[1:]
    count = jnp.sum(lengths).astype(jnp.float32)
    loss = exchange(jnp.full((1, 128), loss, jnp.float32), n, 2, total=True)[0, 0]
    return (out, loss / count)


def solution(mesh):
    return jax.shard_map(
        per_device,
        mesh=mesh,
        in_specs=(P("dp", None), P("dp", None), P(), P(None, None, "dp"), P(None, "dp", None), P()),
        out_specs=(P("dp", None), P()),
        check_vma=False,
    )
```
